32 devices in a mesh: ep: 4 (over y, x), dp: 2 (over core), tp: 4 (over z).
Axes of the slice: x: 2, y: 2, z: 4, core: 2. Of those that a mesh axis runs over, the one named last changes fastest.
Arguments:
- tokens: bfloat16 [192, 7168], P(('ep', 'dp')), may hold values from -6 to 6
- expert_ids: int32 [192, 8], P(('ep', 'dp')), may hold values from 0 to 31, all different within a row; in each aligned block of 24 rows (0 to 23, 24 to 47, ...) at most 8 rows name the same one
- route_weight: float32 [192, 8], P(('ep', 'dp')), may hold values from 0.1 to 0.6
- gate_weight: bfloat16 [32, 7168, 1536], P('ep', None, 'tp'), may hold values from -0.0625 to 0.0625
- up_weight: bfloat16 [32, 7168, 1536], P('ep', None, 'tp'), may hold values from -0.0625 to 0.0625
- down_weight: bfloat16 [32, 1536, 7168], P('ep', 'tp'), may hold values from -0.15625 to 0.15625
Outputs:
- moe_out: bfloat16 [192, 7168], P(('ep', 'dp', 'tp'))
The draws below stay inside these ranges and needn't reach their ends.
Inputs may be any that keep to these rules, and one draw needn't show every extreme that they name: `expert_ids`: each row names 8 different experts. In every aligned block of 24 rows no expert is named by more than 8 rows, a bound that some block reaches.
All inputs are finite; a program needn't handle non-finite values.
Results may differ from the reference program's by a relative error of at most 0.0049.
Values may be sent and summed in bfloat16 or wider, within the bound.
A program may use at most 192 MiB of HBM per device.

```python
import math
import jax
import jax.numpy as jnp
import numpy as np
from jax import lax

D = 7168
FF = 1536
TOP = 8
EXPERTS = 32
TOK_DEV = 24
MOST = 8
TOKENS = 192
N_TP = 4


def shard_levels(stream_key, dims, shards, low, high):
    def one(axis_at, shards_of):
        heights = jax.random.uniform(jax.random.fold_in(jax.random.fold_in(stream_key, 6), axis_at), (shards_of,), jnp.float32, low / len(shards), high / len(shards))
        return jnp.repeat(jnp.exp(heights), dims[axis_at] // shards_of).reshape((-1,) + (1,) * (len(dims) - axis_at - 1))

    level = one(*shards[0])
    for cut in shards[1:]:
        level = level * one(*cut)
    return level


def routed_block(rng, own, number, rows, count, top, reach, lean):
    ranking = jax.random.permutation(rng, count)
    crowded, usual = load_shares(count, rows * top, reach, lean, True), load_shares(count, rows * top, reach, lean, False)
    places = jnp.arange(count)

    def named(lengths, turn):
        used = int((lengths > 0).sum())
        fixed = max(1, used // 4)
        passed = fixed + (places - fixed + turn * (used - fixed)) % max(1, count - fixed)
        return jnp.zeros((count,), jnp.int32).at[ranking[jnp.where(places < fixed, places, passed)]].set(jnp.asarray(lengths, jnp.int32))

    lengths = jnp.where(number % 4 == 0, named(crowded, number // 4), named(usual, number - number // 4 - 1))
    mixed = jax.random.permutation(jax.random.fold_in(own, 3), count)
    giver, taker = mixed[0:count // 2 * 2:2], mixed[1:count // 2 * 2:2]
    room = jnp.minimum(lengths[giver] - 1, reach - lengths[taker]) // 2
    room = jnp.where((giver == ranking[0]) | (taker == ranking[0]) | (lengths[taker] == 0), 0, jnp.maximum(room, 0))
    passed = jax.random.randint(jax.random.fold_in(own, 4), (count // 2,), 0, 1 << 20) % (room + 1)
    lengths = lengths.at[giver].add(-passed).at[taker].add(passed)
    members = jnp.searchsorted(jnp.cumsum(lengths), jnp.arange(rows * top), side="right").astype(jnp.int32)
    grid = members.reshape(top, rows).T
    grid = grid[jax.random.permutation(jax.random.fold_in(own, 1), rows)]
    turn = jax.random.randint(jax.random.fold_in(own, 2), (rows, 1), 0, top)
    return jnp.take_along_axis(grid, (jnp.arange(top)[None, :] + turn) % top, axis=1)


def load_shares(count, total, most, slope, full):
    portions = [(1 << 20) // math.isqrt(grade ** slope) + 1 for grade in range(1, count + 1)]
    largest = most if full else min(most, max(-(-total // count), total * portions[0] // sum(portions)))
    least = 1 if total - largest >= count - 1 else 0
    counts, surplus = [largest] + [least] * (count - 1), total - largest - least * (count - 1)
    while surplus > 0:
        candidates = [i for i in range(1, count) if counts[i] < largest] or [i for i in range(1, count) if counts[i] < most]
        pool, left = sum([portions[i] for i in candidates]), surplus
        for i in candidates:
            addition = min(most - counts[i], max(1, left * portions[i] // pool), surplus)
            counts[i] = counts[i] + addition
            surplus = surplus - addition
    return np.array(counts)


def noise(rng, dims, width, limit, cuts=(), held_as=jnp.bfloat16):
    gain = shard_levels(rng, dims, cuts, -0.22, 0.18) if cuts else 1.0
    result = jax.random.normal(rng, dims, jnp.float32) * width * gain
    return jnp.minimum(jnp.maximum(result, -limit), limit).astype(held_as)


def setup_inputs(seed: int = 0) -> dict:
    arg_keys = jax.random.split(jax.random.key(seed), 7)
    tokens = noise(arg_keys[0], (TOKENS, D), 1.0, 6.0, ((0, 8),))
    expert_ids_keys = jax.random.split(jax.random.fold_in(arg_keys[1], 1), TOKENS // TOK_DEV)
    expert_ids_turns = jax.random.permutation(jax.random.fold_in(arg_keys[1], 3), TOKENS // TOK_DEV)
    expert_ids = jax.vmap(lambda own, number: routed_block(jax.random.fold_in(arg_keys[1], 2), own, number, TOK_DEV, EXPERTS, TOP, MOST, 2))(expert_ids_keys, expert_ids_turns).reshape((TOKENS, TOP))
    route_weight = jnp.clip(0.1 + 0.5 * jax.random.uniform(arg_keys[2], (TOKENS, TOP), jnp.float32) ** shard_levels(arg_keys[2], (TOKENS, TOP), ((0, 8),), -0.2, 0.2), 0.1, 0.6)
    gate_weight = noise(arg_keys[3], (EXPERTS, D, FF), D ** -0.5, 0.0625, ((0, 4), (2, 4)))
    up_weight = noise(arg_keys[4], (EXPERTS, D, FF), D ** -0.5, 0.0625, ((0, 4), (2, 4)))
    down_weight = noise(arg_keys[5], (EXPERTS, FF, D), FF ** -0.5, 0.15625, ((0, 4), (1, 4)))
    return {"tokens": tokens, "expert_ids": expert_ids, "route_weight": route_weight, "gate_weight": gate_weight, "up_weight": up_weight, "down_weight": down_weight}


def run_expert(packed):
    row_data, gate_w, up_w, down_w = packed
    gate_proj = jnp.dot(row_data, gate_w, preferred_element_type=jnp.float32)
    up_proj = jnp.dot(row_data, up_w, preferred_element_type=jnp.float32)
    hidden = (jax.nn.silu(gate_proj) * up_proj).astype(jnp.bfloat16)
    groups = hidden.reshape(hidden.shape[0], N_TP, FF // N_TP).astype(jnp.float32)
    pieces = down_w.reshape(N_TP, FF // N_TP, D).astype(jnp.float32)
    partial_sums = jnp.einsum("cgf,gfd->gcd", groups, pieces)
    return jnp.sum(partial_sums, 0)


def reference(tokens, expert_ids, route_weight, gate_weight, up_weight, down_weight):
    blocks = TOKENS // TOK_DEV
    chosen = expert_ids.reshape(blocks, TOK_DEV * TOP).astype(jnp.int32)
    onehot = (chosen[:, :, None] == jnp.arange(EXPERTS, dtype=jnp.int32)[None, None, :]).astype(jnp.int32)
    earlier = jnp.cumsum(onehot, 1) - onehot
    slot_index = jnp.sum(earlier * onehot, 2).astype(jnp.int32)
    position = (jnp.arange(blocks, dtype=jnp.int32)[:, None] * MOST + slot_index).reshape(-1).astype(jnp.int32)
    chosen_all = chosen.reshape(-1)
    token_index = (jnp.arange(TOKENS * TOP, dtype=jnp.int32) // TOP).astype(jnp.int32)
    capacity = blocks * MOST
    row_table = jnp.full((EXPERTS, capacity), TOKENS, jnp.int32).at[chosen_all, position].set(token_index)
    padded = jnp.concatenate([tokens, jnp.zeros((1, D), jnp.bfloat16)], 0)
    gathered_in = padded[row_table]
    expert_out = lax.map(run_expert, (gathered_in, gate_weight, up_weight, down_weight))
    picked = expert_out[chosen_all, position].reshape(TOKENS, TOP, D)
    mixed = jnp.sum(route_weight[:, :, None] * picked, 1)
    return mixed.astype(jnp.bfloat16)
```

```python
from functools import partial

import jax
import jax.numpy as jnp
from jax import lax
from jax.experimental import pallas as pl
from jax.experimental.pallas import tpu as pltpu
from jax.sharding import PartitionSpec as P

TOP = 8
EXPERTS = 32
MOST = 8
MESH = pl.DeviceIdType.MESH
VMEM_BYTES = 67_000_000
AHEAD = 4
EARLY = 5
LAGS = (3, 5, 9)


def expert_block(received, gate_weight, up_weight, down_weight):
    ep_size = lax.axis_size("ep")
    local_count = gate_weight.shape[0]
    slot_count = received.shape[1]
    width = received.shape[2]
    shaped = received.reshape(ep_size, local_count, slot_count, width)
    gate_proj = jnp.einsum(
        "sxmd,xdf->sxmf", shaped, gate_weight, preferred_element_type=jnp.float32
    )
    up_proj = jnp.einsum("sxmd,xdf->sxmf", shaped, up_weight, preferred_element_type=jnp.float32)
    hidden = (jax.nn.silu(gate_proj) * up_proj).astype(jnp.bfloat16)
    partial_rows = jnp.einsum(
        "sxmf,xfd->sxmd", hidden, down_weight, preferred_element_type=jnp.float32
    )
    partial_rows = partial_rows.reshape(ep_size * local_count, slot_count, width)
    return lax.all_to_all(partial_rows, "ep", split_axis=0, concat_axis=0, tiled=True)


def build_rows(source, per_token):
    width = source.shape[1]
    dispatch = jnp.any(per_token, 1).astype(jnp.bfloat16)
    outgoing = jnp.einsum("tp,td->pd", dispatch, source, preferred_element_type=jnp.float32).astype(
        jnp.bfloat16
    )
    return outgoing.reshape(EXPERTS, MOST, width)


def combine_rows(returned, per_token, route_weight):
    weight_table = jnp.sum(per_token.astype(jnp.float32) * route_weight[:, :, None], 1)
    combined = jnp.dot(weight_table, returned, precision=lax.Precision.HIGHEST)
    return combined


def per_device(tokens, expert_ids, route_weight, gate_weight, up_weight, down_weight):
    rows_here = tokens.shape[0]
    width = tokens.shape[1]
    capacity = EXPERTS * MOST
    chosen = expert_ids.reshape(-1)
    onehot = (chosen[:, None] == jnp.arange(EXPERTS, dtype=jnp.int32)[None, :]).astype(jnp.int32)
    earlier = jnp.cumsum(onehot, 0) - onehot
    slot_index = jnp.sum(earlier * onehot, 1)
    position = chosen * MOST + slot_index
    matches = position[:, None] == jnp.arange(capacity, dtype=jnp.int32)[None, :]
    per_token = matches.reshape(rows_here, TOP, capacity)
    outgoing = build_rows(tokens, per_token)
    worker = partial(
        expert_block, gate_weight=gate_weight, up_weight=up_weight, down_weight=down_weight
    )
    returned = worker(lax.all_to_all(outgoing, "ep", split_axis=0, concat_axis=0, tiled=True))
    returned = returned.reshape(capacity, width)
    combined = combine_rows(returned, per_token, route_weight)
    summed = lax.psum_scatter(combined, "tp", scatter_dimension=0, tiled=True)
    return summed.astype(jnp.bfloat16)


def xor_bit(index, bit):
    return index + bit - 2 * bit * ((index // bit) % 2)


def xor_any(index, mask):
    bit = 1
    while bit <= mask:
        if mask & bit:
            index = xor_bit(index, bit)
        bit *= 2
    return index


def rotated(bits, turn):
    turn %= len(bits)
    return bits[turn:] + bits[:turn]


def moe_kernel(
    n_ep, n_tp, ring, early,
    tok_ref, ids_ref, rw_ref, gate_ref, up_ref, down_ref,
    out_ref,
    xs, ids_own, rw_own, ids_all, rw_all, gu, dn, acc, hid, own, out0, in0, out1, in1,
    last_keep, last_out, last_in,
    in_sem, small_send, small_recv, ag_send, ag_recv, gu_sem, dn_sem, hid_send, hid_recv,
    fold_send, fold_recv, last_send, last_recv,
):
    ep, dp, tp = lax.axis_index("ep"), lax.axis_index("dp"), lax.axis_index("tp")
    rows = tok_ref.shape[0]
    chunks, sides, groups, _, step_width = xs.shape
    units = gate_ref.shape[2]
    pairs = acc.shape[0]
    depth = gu.shape[1]
    items = chunks * pairs
    experts = 2 * pairs
    blocks = dn.shape[0]
    wide = dn.shape[3]
    half = blocks * wide
    sub = wide // 2
    total_rows = groups * rows
    half_rows = n_ep * rows
    out_rows = rows // n_tp
    bits = [1 << i for i in range(n_ep.bit_length() - 1)]
    first_expert = dp * experts
    other_first = (1 - dp) * experts
    sibling = {"dp": 1 - dp}
    column = dp * half

    def arrived(ref, sem):
        pltpu.make_async_copy(ref, ref, sem).wait()

    def start_gu(item):
        chunk, pair = item // pairs, item % pairs
        slot = item % ring
        for e in range(2):
            for at, ref in enumerate((gate_ref, up_ref)):
                pltpu.make_async_copy(
                    ref.at[first_expert + 2 * pair + e, pl.ds(chunk * depth, depth), :],
                    gu.at[slot, :, pl.ds((2 * e + at) * units, units)],
                    gu_sem.at[slot],
                ).start()

    def start_dn(n):
        cols = pl.ds(pl.multiple_of(column + n * wide, 128), wide)
        for at, first in enumerate((first_expert, other_first)):
            pltpu.make_async_copy(
                down_ref.at[pl.ds(first, experts), :, cols],
                dn.at[n, pl.ds(at * experts, experts)],
                dn_sem.at[n],
            ).start()

    for chunk in range(chunks):
        for side in range(sides):
            pltpu.make_async_copy(
                tok_ref.at[:, pl.ds((chunk * sides + side) * step_width, step_width)],
                xs.at[chunk, side, 0],
                in_sem.at[0],
            ).start()
    small_in = [
        pltpu.make_async_copy(ids_ref, ids_own, in_sem.at[1]),
        pltpu.make_async_copy(rw_ref, rw_own, in_sem.at[2]),
    ]
    for copy in small_in:
        copy.start()

    group = [(q, other) for other in range(2) for q in range(n_ep) if (q, other) != (0, 0)]
    barrier = pltpu.get_barrier_semaphore()
    for q, other in group:
        pl.semaphore_signal(
            barrier, inc=1, device_id={"ep": xor_any(ep, q), "dp": 1 - dp if other else dp},
            device_id_type=MESH,
        )
    for step in range(1, n_tp):
        for to in (dp, 1 - dp):
            pl.semaphore_signal(
                barrier, inc=1, device_id={"dp": to, "tp": lax.rem(tp + step, n_tp)},
                device_id_type=MESH,
            )
    with jax.named_scope("inwait"):
        arrived(xs.at[:, :, 0], in_sem.at[0])
        for copy in small_in:
            copy.wait()
    for item in range(min(early, items)):
        start_gu(item)
    ids_all[:rows, :] = ids_own[...].T
    rw_all[:rows, :] = rw_own[...].T
    with jax.named_scope("barrier"):
        pl.semaphore_wait(barrier, len(group) + 2 * (n_tp - 1))

    def send(src, dst, send_sem, recv_sem, device):
        pltpu.make_async_remote_copy(
            src_ref=src, dst_ref=dst, send_sem=send_sem, recv_sem=recv_sem, device_id=device,
            device_id_type=MESH,
        ).start()

    def gather(chunk, step):
        for side in range(sides):
            order = rotated(bits, side)
            have = [0]
            for bit in order[:step]:
                have = have + [q ^ bit for q in have]
            bit = order[step]
            for q in have:
                send(
                    xs.at[chunk, side, q], xs.at[chunk, side, q ^ bit],
                    ag_send, ag_recv.at[chunk, step], {"ep": xor_bit(ep, bit)},
                )

    def gathered(chunk, step):
        with jax.named_scope(f"ag{step}#k={chunk}"):
            arrived(xs.at[chunk, :, pl.ds(0, 1 << step)], ag_recv.at[chunk, step])

    def gather_pair(chunk):
        gathered(chunk, 1)
        send(
            xs.at[chunk, :, pl.ds(0, n_ep)], xs.at[chunk, :, pl.ds(n_ep, n_ep)],
            ag_send, ag_recv.at[chunk, 2], sibling,
        )

    lead = min(AHEAD, chunks)
    for chunk in range(lead):
        gather(chunk, 0)
    for q, other in group:
        device = {"ep": xor_any(ep, q), "dp": 1 - dp if other else dp}
        row = (other * n_ep + q) * rows
        for kind, ref in enumerate((ids_all, rw_all)):
            send(
                ref.at[pl.ds(0, rows), :], ref.at[pl.ds(row, rows), :],
                small_send.at[kind], small_recv.at[kind], device,
            )
    asked = 0

    def relay():
        nonlocal asked
        if asked < chunks:
            gathered(asked, 0)
            gather(asked, 1)
            if asked + lead < chunks:
                gather(asked + lead, 0)
            asked += 1

    for _ in range(lead):
        relay()
    for item in range(early, min(ring, items)):
        start_gu(item)

    def product(chunk, pair):
        slot = (chunk * pairs + pair) % ring
        value = 0.0
        for side in range(sides):
            value += jnp.dot(
                xs[chunk, side].reshape(total_rows, step_width),
                gu[slot, side * step_width : (side + 1) * step_width],
                preferred_element_type=jnp.float32,
            )
        return value

    base = ep * (2 * experts) + first_expert
    started = 0
    gather_pair(0)
    for chunk in range(chunks):
        relay()
        if chunk + 1 < chunks:
            gather_pair(chunk + 1)
        with jax.named_scope(f"pairwait#k={chunk}"):
            arrived(xs.at[chunk, :, pl.ds(n_ep, n_ep)], ag_recv.at[chunk, 2])
        if chunk + 1 < chunks:
            with jax.named_scope(f"guwait#k={chunk}"):
                for pair in range(pairs):
                    slot = (chunk * pairs + pair) % ring
                    arrived(gu.at[slot], gu_sem.at[slot])
            with jax.named_scope(f"gateup#k={chunk}"):
                for pair in range(pairs):
                    value = product(chunk, pair)
                    if chunk == 0:
                        acc[pair] = value
                    else:
                        acc[pair] += value
            for pair in range(pairs):
                item = chunk * pairs + pair + ring
                if item < items:
                    start_gu(item)
            while started < blocks and started < (chunk + 1) * pairs - (items - ring) + 2:
                start_dn(started)
                started += 1
    while started < blocks:
        start_dn(started)
        started += 1

    for kind, ref in enumerate((ids_all, rw_all)):
        arrived(ref.at[pl.ds(rows, total_rows - rows)], small_recv.at[kind])
    for pair in range(pairs):
        with jax.named_scope(f"last#p={pair}"):
            slot = ((chunks - 1) * pairs + pair) % ring
            arrived(gu.at[slot], gu_sem.at[slot])
            value = product(chunks - 1, pair)
            if chunks > 1:
                value += acc[pair]
            for e in range(2):
                weight = jnp.sum(
                    jnp.where(ids_all[...] == base + 2 * pair + e, rw_all[...], 0.0), 1, keepdims=True
                )
                gate = value[:, 2 * e * units : (2 * e + 1) * units]
                up = value[:, (2 * e + 1) * units : (2 * e + 2) * units]
                hidden = gate / (1.0 + jnp.exp(-gate)) * up * weight
                hid[pair, :, e * units : (e + 1) * units] = hidden.astype(jnp.bfloat16)
        for at in range(2):
            send(
                hid.at[pair, pl.ds(at * half_rows, half_rows), :],
                hid.at[pairs + pair, pl.ds((1 - at) * half_rows, half_rows), :],
                hid_send, hid_recv.at[pair], sibling,
            )

    def split(side, step):
        kept = list(range(n_ep))
        order = rotated(bits, side)
        for bit in order[:step]:
            kept = [q for q in kept if not q & bit]
        bit = order[step]
        return bit, [q for q in kept if not q & bit], [q for q in kept if q & bit]

    def fold_send_to(n, side, step):
        bit, _, _ = split(side, step)
        src, dst = ((out0, in0), (out1, in1))[step]
        send(
            src.at[n, side], dst.at[n, side], fold_send.at[step], fold_recv.at[n, step],
            {"ep": xor_bit(ep, bit)},
        )

    def down(n, low, high):
        value = 0.0
        for p in range(low, high):
            value += jnp.dot(
                hid[p], dn[n, 2 * p : 2 * p + 2].reshape(2 * units, wide),
                preferred_element_type=jnp.float32,
            )
        return value

    def store0(n, value):
        for side in range(2):
            _, kept, away = split(side, 0)
            cols = slice(side * sub, (side + 1) * sub)
            for d in range(2):
                for i, q in enumerate(away):
                    row = d * half_rows + q * rows
                    out0[n, side, d, i] = value[row : row + rows, cols].astype(jnp.bfloat16)
                for i, q in enumerate(kept):
                    row = d * half_rows + q * rows
                    own[n, side, d, i] = value[row : row + rows, cols]

    def fold0(n):
        for side in range(2):
            fold_send_to(n, side, 0)

    def fold1(n):
        arrived(in0.at[n], fold_recv.at[n, 0])
        for side in range(2):
            _, held, _ = split(side, 0)
            _, kept, away = split(side, 1)
            at_away, at_kept = held.index(away[0]), held.index(kept[0])
            for d in range(2):
                total = own[n, side, d, at_away] + in0[n, side, d, at_away].astype(jnp.float32)
                out1[n, side, d] = total.astype(jnp.bfloat16)
                own[n, side, d, at_kept] += in0[n, side, d, at_kept].astype(jnp.float32)
        for side in range(2):
            fold_send_to(n, side, 1)

    def fold2(n):
        arrived(in1.at[n], fold_recv.at[n, 1])
        for side in range(2):
            _, held, _ = split(side, 0)
            at_kept = held.index(0)
            cols = slice(side * sub, (side + 1) * sub)
            for d in range(2):
                total = own[n, side, d, at_kept] + in1[n, side, d].astype(jnp.float32)
                for t in range(n_tp):
                    piece = total[t * out_rows : (t + 1) * out_rows]
                    if d == 0:
                        last_keep[n, t, :, cols] = piece
                    last_out[n, d, t, :, cols] = piece.astype(jnp.bfloat16)
        for step in range(n_tp):
            peer = lax.rem(tp + step, n_tp)
            for other, to in enumerate((dp, 1 - dp)):
                if step or other:
                    send(
                        last_out.at[n, other, peer], last_in.at[n, step * 2 + other - 1],
                        last_send, last_recv.at[n], {"dp": to, "tp": peer},
                    )

    def finish(n):
        arrived(last_in.at[n], last_recv.at[n])
        for other in range(2):
            value = 0.0 if other else last_keep[n, tp]
            for step in range(n_tp):
                if step or other:
                    value += last_in[n, step * 2 + other - 1].astype(jnp.float32)
            start = (1 - dp if other else dp) * half + n * wide
            out_ref[:, pl.ds(pl.multiple_of(start, 128), wide)] = value.astype(out_ref.dtype)

    def stage(n, fn, name):
        if 0 <= n < blocks:
            with jax.named_scope(f"{name}#n={n}"):
                fn(n)

    first = min(2, blocks, pairs)
    for n in range(first):
        with jax.named_scope(f"down_own#n={n}"):
            arrived(dn.at[n], dn_sem.at[n])
            acc[n, :, :wide] = down(n, 0, pairs)
    with jax.named_scope("hidwait"):
        for pair in range(pairs):
            arrived(hid.at[pairs + pair], hid_recv.at[pair])
    for turn in range(blocks + LAGS[2]):
        if turn < blocks:
            with jax.named_scope(f"down#n={turn}"):
                if turn < first:
                    value = down(turn, pairs, 2 * pairs) + acc[turn, :, :wide]
                else:
                    arrived(dn.at[turn], dn_sem.at[turn])
                    value = down(turn, 0, 2 * pairs)
                store0(turn, value)
        stage(turn - LAGS[0], fold1, "fold1")
        stage(turn, fold0, "fold0")
        stage(turn - LAGS[1], fold2, "fold2")
        stage(turn - LAGS[2], finish, "finish")
    with jax.named_scope("tailsend"):
        arrived(xs.at[:, :, pl.ds(0, groups - 1)], ag_send)
        for kind, ref in enumerate((ids_all, rw_all)):
            arrived(ref.at[pl.ds(rows, total_rows - rows)], small_send.at[kind])
        arrived(hid.at[pl.ds(0, pairs)], hid_send)
        arrived(out0, fold_send.at[0])
        arrived(out1, fold_send.at[1])
        arrived(last_in, last_send)


def fused_plan(mesh, rows, width, local_count, units):
    n_ep, n_dp, n_tp = (mesh.shape[a] for a in ("ep", "dp", "tp"))
    if n_dp != 2 or local_count % 4 or n_ep != 4 or rows % 8 or rows % n_tp:
        return None
    if units % 128 or width % 1024:
        return None
    pairs = local_count // 4
    chunks = width // 1024
    total_rows = 2 * n_ep * rows
    hidden = local_count * units
    slot = 1024 * 4 * units * 2
    pad = -(-(rows // n_tp) // 8) * 8
    held = total_rows * width * 2 + hidden * width + pairs * total_rows * 4 * units * 4
    held += total_rows * hidden * 2 + (total_rows // 2) * (width // 2) * 12
    held += pad * width * (n_tp * 6 + 8 * n_tp) + 5_000_000
    ring = min(chunks * pairs, (VMEM_BYTES - held) // slot)
    if ring < 2 * pairs or pairs < 2 or 4 * units < 512:
        return None
    return chunks, pairs, ring


def fused(mesh, plan, tokens, expert_ids, route_weight, gate_weight, up_weight, down_weight):
    chunks, pairs, ring = plan
    n_ep, n_tp = mesh.shape["ep"], mesh.shape["tp"]
    rows, width = tokens.shape
    units = gate_weight.shape[2]
    wide = 512
    blocks = width // 2 // wide
    depth = width // chunks
    total_rows = 2 * n_ep * rows
    out_rows = rows // n_tp
    top = expert_ids.shape[1]
    sub = wide // 2
    dma = pltpu.SemaphoreType.DMA
    f32, bf16 = jnp.float32, jnp.bfloat16
    return pl.pallas_call(
        partial(moe_kernel, n_ep, n_tp, ring, min(EARLY, ring)),
        out_shape=jax.ShapeDtypeStruct((out_rows, width), bf16),
        in_specs=[pl.BlockSpec(memory_space=pltpu.HBM)] * 6,
        out_specs=pl.BlockSpec(memory_space=pltpu.VMEM),
        scratch_shapes=[
            pltpu.VMEM((chunks, 2, 2 * n_ep, rows, depth // 2), bf16),
            pltpu.VMEM((top, rows), jnp.int32),
            pltpu.VMEM((top, rows), f32),
            pltpu.VMEM((total_rows, top), jnp.int32),
            pltpu.VMEM((total_rows, top), f32),
            pltpu.VMEM((ring, depth, 4 * units), bf16),
            pltpu.VMEM((blocks, 4 * pairs, units, wide), bf16),
            pltpu.VMEM((pairs, total_rows, 4 * units), f32),
            pltpu.VMEM((2 * pairs, total_rows, 2 * units), bf16),
            pltpu.VMEM((blocks, 2, 2, n_ep // 2, rows, sub), f32),
            pltpu.VMEM((blocks, 2, 2, n_ep // 2, rows, sub), bf16),
            pltpu.VMEM((blocks, 2, 2, n_ep // 2, rows, sub), bf16),
            pltpu.VMEM((blocks, 2, 2, rows, sub), bf16),
            pltpu.VMEM((blocks, 2, 2, rows, sub), bf16),
            pltpu.VMEM((blocks, n_tp, out_rows, wide), f32),
            pltpu.VMEM((blocks, 2, n_tp, out_rows, wide), bf16),
            pltpu.VMEM((blocks, 2 * n_tp - 1, out_rows, wide), bf16),
            dma((3,)),
            dma((2,)),
            dma((2,)),
            dma,
            dma((chunks, 3)),
            dma((ring,)),
            dma((blocks,)),
            dma,
            dma((pairs,)),
            dma((2,)),
            dma((blocks, 2)),
            dma,
            dma((blocks,)),
        ],
        compiler_params=pltpu.CompilerParams(
            collective_id=0, has_side_effects=True, vmem_limit_bytes=VMEM_BYTES
        ),
    )(tokens, expert_ids.T, route_weight.T, gate_weight, up_weight, down_weight)


def solution(mesh):
    in_specs = (
        P(("ep", "dp"), None),
        P(("ep", "dp"), None),
        P(("ep", "dp"), None),
        P("ep", None, "tp"),
        P("ep", None, "tp"),
        P("ep", "tp", None),
    )
    out_specs = P(("ep", "dp", "tp"), None)

    def body(*arrays):
        rows, width = arrays[0].shape
        local_count, _, units = arrays[3].shape
        plan = fused_plan(mesh, rows, width, local_count, units)
        if plan is None:
            return per_device(*arrays)
        return fused(mesh, plan, *arrays)

    return jax.shard_map(body, mesh=mesh, in_specs=in_specs, out_specs=out_specs, check_vma=False)
```

```python
from functools import partial

import jax
import jax.numpy as jnp
from jax import lax
from jax.experimental import pallas as pl
from jax.experimental.pallas import tpu as pltpu
from jax.sharding import PartitionSpec as P

TOP = 8
EXPERTS = 32
MOST = 8
MESH = pl.DeviceIdType.MESH
VMEM_BYTES = 67_000_000
AHEAD = 4
EARLY = 5
LAGS = (3, 5, 9)
Z_TURNS = (7, 9, 11)


def expert_block(received, gate_weight, up_weight, down_weight):
    ep_size = lax.axis_size("ep")
    local_count = gate_weight.shape[0]
    slot_count = received.shape[1]
    width = received.shape[2]
    shaped = received.reshape(ep_size, local_count, slot_count, width)
    gate_proj = jnp.einsum(
        "sxmd,xdf->sxmf", shaped, gate_weight, preferred_element_type=jnp.float32
    )
    up_proj = jnp.einsum("sxmd,xdf->sxmf", shaped, up_weight, preferred_element_type=jnp.float32)
    hidden = (jax.nn.silu(gate_proj) * up_proj).astype(jnp.bfloat16)
    partial_rows = jnp.einsum(
        "sxmf,xfd->sxmd", hidden, down_weight, preferred_element_type=jnp.float32
    )
    partial_rows = partial_rows.reshape(ep_size * local_count, slot_count, width)
    return lax.all_to_all(partial_rows, "ep", split_axis=0, concat_axis=0, tiled=True)


def build_rows(source, per_token):
    width = source.shape[1]
    dispatch = jnp.any(per_token, 1).astype(jnp.bfloat16)
    outgoing = jnp.einsum("tp,td->pd", dispatch, source, preferred_element_type=jnp.float32).astype(
        jnp.bfloat16
    )
    return outgoing.reshape(EXPERTS, MOST, width)


def combine_rows(returned, per_token, route_weight):
    weight_table = jnp.sum(per_token.astype(jnp.float32) * route_weight[:, :, None], 1)
    combined = jnp.dot(weight_table, returned, precision=lax.Precision.HIGHEST)
    return combined


def per_device(tokens, expert_ids, route_weight, gate_weight, up_weight, down_weight):
    rows_here = tokens.shape[0]
    width = tokens.shape[1]
    capacity = EXPERTS * MOST
    chosen = expert_ids.reshape(-1)
    onehot = (chosen[:, None] == jnp.arange(EXPERTS, dtype=jnp.int32)[None, :]).astype(jnp.int32)
    earlier = jnp.cumsum(onehot, 0) - onehot
    slot_index = jnp.sum(earlier * onehot, 1)
    position = chosen * MOST + slot_index
    matches = position[:, None] == jnp.arange(capacity, dtype=jnp.int32)[None, :]
    per_token = matches.reshape(rows_here, TOP, capacity)
    outgoing = build_rows(tokens, per_token)
    worker = partial(
        expert_block, gate_weight=gate_weight, up_weight=up_weight, down_weight=down_weight
    )
    returned = worker(lax.all_to_all(outgoing, "ep", split_axis=0, concat_axis=0, tiled=True))
    returned = returned.reshape(capacity, width)
    combined = combine_rows(returned, per_token, route_weight)
    summed = lax.psum_scatter(combined, "tp", scatter_dimension=0, tiled=True)
    return summed.astype(jnp.bfloat16)


def xor_bit(index, bit):
    return index + bit - 2 * bit * ((index // bit) % 2)


def xor_any(index, mask):
    bit = 1
    while bit <= mask:
        if mask & bit:
            index = xor_bit(index, bit)
        bit *= 2
    return index


def rotated(bits, turn):
    turn %= len(bits)
    return bits[turn:] + bits[:turn]


def moe_kernel(
    n_ep, n_tp, ring, early,
    tok_ref, ids_ref, rw_ref, gate_ref, up_ref, down_ref,
    out_ref,
    xs, ids_own, rw_own, ids_all, rw_all, gu, dn, acc, hid, own, out0, in0, out1, in1,
    last_keep, last_out, last_in,
    zkeep, zout, zin, zown, zout0, zin0, zout1, zin1, zlast_keep, zlast_out, zlast_in,
    in_sem, small_send, small_recv, ag_send, ag_recv, gu_sem, dn_sem, hid_send, hid_recv,
    fold_send, fold_recv, last_send, last_recv, out_v, out_sem,
    zsend, zrecv, zfold_send, zfold_recv, zlast_send, zlast_recv,
):
    ep, dp, tp = lax.axis_index("ep"), lax.axis_index("dp"), lax.axis_index("tp")
    rows = tok_ref.shape[0]
    chunks, sides, groups, _, step_width = xs.shape
    units = gate_ref.shape[2]
    pairs = acc.shape[0]
    depth = gu.shape[1]
    items = chunks * pairs
    experts = 2 * pairs
    blocks = dn.shape[0]
    wide = dn.shape[3]
    half = blocks * wide
    sub = wide // 2
    total_rows = groups * rows
    half_rows = n_ep * rows
    out_rows = rows // n_tp
    bits = [1 << i for i in range(n_ep.bit_length() - 1)]
    first_expert = dp * experts
    other_first = (1 - dp) * experts
    sibling = {"dp": 1 - dp}
    column = dp * half
    z_block = 1

    def arrived(ref, sem):
        pltpu.make_async_copy(ref, ref, sem).wait()

    def start_gu(item):
        chunk, pair = item // pairs, item % pairs
        slot = item % ring
        for e in range(2):
            for at, ref in enumerate((gate_ref, up_ref)):
                pltpu.make_async_copy(
                    ref.at[first_expert + 2 * pair + e, pl.ds(chunk * depth, depth), :],
                    gu.at[slot, :, pl.ds((2 * e + at) * units, units)],
                    gu_sem.at[slot],
                ).start()

    def start_dn(n):
        cols = pl.ds(pl.multiple_of(column + n * wide, 128), wide)
        for at, first in enumerate((first_expert, other_first)):
            pltpu.make_async_copy(
                down_ref.at[pl.ds(first, experts), :, cols],
                dn.at[n, pl.ds(at * experts, experts)],
                dn_sem.at[n],
            ).start()

    for chunk in range(chunks):
        for side in range(sides):
            pltpu.make_async_copy(
                tok_ref.at[:, pl.ds((chunk * sides + side) * step_width, step_width)],
                xs.at[chunk, side, 0],
                in_sem.at[0],
            ).start()
    small_in = [
        pltpu.make_async_copy(ids_ref, ids_own, in_sem.at[1]),
        pltpu.make_async_copy(rw_ref, rw_own, in_sem.at[2]),
    ]
    for copy in small_in:
        copy.start()

    group = [(q, other) for other in range(2) for q in range(n_ep) if (q, other) != (0, 0)]
    barrier = pltpu.get_barrier_semaphore()
    for q, other in group:
        pl.semaphore_signal(
            barrier, inc=1, device_id={"ep": xor_any(ep, q), "dp": 1 - dp if other else dp},
            device_id_type=MESH,
        )
    for step in range(1, n_tp):
        for to in (dp, 1 - dp):
            pl.semaphore_signal(
                barrier, inc=1, device_id={"dp": to, "tp": lax.rem(tp + step, n_tp)},
                device_id_type=MESH,
            )
    with jax.named_scope("inwait"):
        arrived(xs.at[:, :, 0], in_sem.at[0])
        for copy in small_in:
            copy.wait()
    for item in range(min(early, items)):
        start_gu(item)
    ids_all[:rows, :] = ids_own[...].T
    rw_all[:rows, :] = rw_own[...].T
    with jax.named_scope("barrier"):
        pl.semaphore_wait(barrier, len(group) + 2 * (n_tp - 1))

    def send(src, dst, send_sem, recv_sem, device):
        pltpu.make_async_remote_copy(
            src_ref=src, dst_ref=dst, send_sem=send_sem, recv_sem=recv_sem, device_id=device,
            device_id_type=MESH,
        ).start()

    def gather(chunk, step):
        for side in range(sides):
            order = rotated(bits, side)
            have = [0]
            for bit in order[:step]:
                have = have + [q ^ bit for q in have]
            bit = order[step]
            for q in have:
                send(
                    xs.at[chunk, side, q], xs.at[chunk, side, q ^ bit],
                    ag_send, ag_recv.at[chunk, step], {"ep": xor_bit(ep, bit)},
                )

    def gathered(chunk, step):
        with jax.named_scope(f"ag{step}#k={chunk}"):
            arrived(xs.at[chunk, :, pl.ds(0, 1 << step)], ag_recv.at[chunk, step])

    def gather_pair(chunk):
        gathered(chunk, 1)
        send(
            xs.at[chunk, :, pl.ds(0, n_ep)], xs.at[chunk, :, pl.ds(n_ep, n_ep)],
            ag_send, ag_recv.at[chunk, 2], sibling,
        )

    lead = min(AHEAD, chunks)
    for chunk in range(lead):
        gather(chunk, 0)
    def share_routes():
        for q, other in group:
            device = {"ep": xor_any(ep, q), "dp": 1 - dp if other else dp}
            row = (other * n_ep + q) * rows
            for kind, ref in enumerate((ids_all, rw_all)):
                send(
                    ref.at[pl.ds(0, rows), :], ref.at[pl.ds(row, rows), :],
                    small_send.at[kind], small_recv.at[kind], device,
                )

    asked = 0

    def relay():
        nonlocal asked
        if asked < chunks:
            gathered(asked, 0)
            gather(asked, 1)
            if asked + lead < chunks:
                gather(asked + lead, 0)
            asked += 1
            if asked == chunks:
                share_routes()

    for _ in range(lead):
        relay()
    for item in range(early, min(ring, items)):
        start_gu(item)

    def product(chunk, pair):
        slot = (chunk * pairs + pair) % ring
        value = 0.0
        for side in range(sides):
            value += jnp.dot(
                xs[chunk, side].reshape(total_rows, step_width),
                gu[slot, side * step_width : (side + 1) * step_width],
                preferred_element_type=jnp.float32,
            )
        return value

    base = ep * (2 * experts) + first_expert
    started = 0
    gather_pair(0)
    for chunk in range(chunks):
        relay()
        if chunk + 1 < chunks:
            gather_pair(chunk + 1)
        with jax.named_scope(f"pairwait#k={chunk}"):
            arrived(xs.at[chunk, :, pl.ds(n_ep, n_ep)], ag_recv.at[chunk, 2])
        if chunk + 1 < chunks:
            with jax.named_scope(f"guwait#k={chunk}"):
                for pair in range(pairs):
                    slot = (chunk * pairs + pair) % ring
                    arrived(gu.at[slot], gu_sem.at[slot])
            with jax.named_scope(f"gateup#k={chunk}"):
                for pair in range(pairs):
                    value = product(chunk, pair)
                    if chunk == 0:
                        acc[pair] = value
                    else:
                        acc[pair] += value
            for pair in range(pairs):
                item = chunk * pairs + pair + ring
                if item < items:
                    start_gu(item)
            while started < blocks and started < (chunk + 1) * pairs - (items - ring) + 2:
                start_dn(started)
                started += 1
    while started < blocks:
        start_dn(started)
        started += 1

    for kind, ref in enumerate((ids_all, rw_all)):
        arrived(ref.at[pl.ds(rows, total_rows - rows)], small_recv.at[kind])
    for pair in range(pairs):
        with jax.named_scope(f"last#p={pair}"):
            slot = ((chunks - 1) * pairs + pair) % ring
            arrived(gu.at[slot], gu_sem.at[slot])
            value = product(chunks - 1, pair)
            if chunks > 1:
                value += acc[pair]
            for e in range(2):
                weight = jnp.sum(
                    jnp.where(ids_all[...] == base + 2 * pair + e, rw_all[...], 0.0), 1, keepdims=True
                )
                gate = value[:, 2 * e * units : (2 * e + 1) * units]
                up = value[:, (2 * e + 1) * units : (2 * e + 2) * units]
                hidden = gate / (1.0 + jnp.exp(-gate)) * up * weight
                hid[pair, :, e * units : (e + 1) * units] = hidden.astype(jnp.bfloat16)
        for at in range(2):
            send(
                hid.at[pair, pl.ds(at * half_rows, half_rows), :],
                hid.at[pairs + pair, pl.ds((1 - at) * half_rows, half_rows), :],
                hid_send, hid_recv.at[pair], sibling,
            )

    def split(side, step):
        kept = list(range(n_ep))
        order = rotated(bits, side)
        for bit in order[:step]:
            kept = [q for q in kept if not q & bit]
        bit = order[step]
        return bit, [q for q in kept if not q & bit], [q for q in kept if q & bit]

    def fold_send_to(n, side, step):
        bit, _, _ = split(side, step)
        src, dst = ((out0, in0), (out1, in1))[step]
        send(
            src.at[n, side], dst.at[n, side], fold_send.at[step], fold_recv.at[n, step],
            {"ep": xor_bit(ep, bit)},
        )

    def down(n, low, high):
        value = 0.0
        for p in range(low, high):
            value += jnp.dot(
                hid[p], dn[n, 2 * p : 2 * p + 2].reshape(2 * units, wide),
                preferred_element_type=jnp.float32,
            )
        return value

    def store0(n, value):
        for side in range(2):
            _, kept, away = split(side, 0)
            cols = slice(side * sub, (side + 1) * sub)
            for d in range(2):
                for i, q in enumerate(away):
                    row = d * half_rows + q * rows
                    out0[n, side, d, i] = value[row : row + rows, cols].astype(jnp.bfloat16)
                for i, q in enumerate(kept):
                    row = d * half_rows + q * rows
                    own[n, side, d, i] = value[row : row + rows, cols]

    def fold0(n):
        for side in range(2):
            fold_send_to(n, side, 0)

    def fold1(n):
        arrived(in0.at[n], fold_recv.at[n, 0])
        for side in range(2):
            _, held, _ = split(side, 0)
            _, kept, away = split(side, 1)
            at_away, at_kept = held.index(away[0]), held.index(kept[0])
            for d in range(2):
                total = own[n, side, d, at_away] + in0[n, side, d, at_away].astype(jnp.float32)
                out1[n, side, d] = total.astype(jnp.bfloat16)
                own[n, side, d, at_kept] += in0[n, side, d, at_kept].astype(jnp.float32)
        for side in range(2):
            fold_send_to(n, side, 1)

    def fold2(n):
        arrived(in1.at[n], fold_recv.at[n, 1])
        for side in range(2):
            _, held, _ = split(side, 0)
            at_kept = held.index(0)
            cols = slice(side * sub, (side + 1) * sub)
            for d in range(2):
                total = own[n, side, d, at_kept] + in1[n, side, d].astype(jnp.float32)
                for t in range(n_tp):
                    piece = total[t * out_rows : (t + 1) * out_rows]
                    if d == 0:
                        last_keep[n, t, :, cols] = piece
                    last_out[n, d, t, :, cols] = piece.astype(jnp.bfloat16)
        for step in range(n_tp):
            peer = lax.rem(tp + step, n_tp)
            for other, to in enumerate((dp, 1 - dp)):
                if step or other:
                    send(
                        last_out.at[n, other, peer], last_in.at[n, step * 2 + other - 1],
                        last_send, last_recv.at[n], {"dp": to, "tp": peer},
                    )

    def put(start, value):
        cols = pl.ds(pl.multiple_of(start, 128), wide)
        out_v[:, cols] = value.astype(out_ref.dtype)
        pltpu.make_async_copy(out_v.at[:, cols], out_ref.at[:, cols], out_sem).start()

    def z_store(value):
        for t in range(n_tp):
            for g in range(groups):
                row = g * rows + t * out_rows
                piece = value[row : row + out_rows]
                zkeep[t, g] = piece
                zout[t, g] = piece.astype(jnp.bfloat16)
        for step in range(1, n_tp):
            peer = lax.rem(tp + step, n_tp)
            send(zout.at[peer], zin.at[step - 1], zsend, zrecv, {"tp": peer})

    def z_fold(src, dst, step):
        for side in range(2):
            bit, _, _ = split(side, step)
            send(
                src.at[side], dst.at[side], zfold_send.at[step], zfold_recv.at[step],
                {"ep": xor_bit(ep, bit)},
            )

    def z_fold0():
        arrived(zin, zrecv)
        for d in range(2):
            for q in range(n_ep):
                total = zkeep[tp, d * n_ep + q]
                for t in range(n_tp - 1):
                    total += zin[t, d * n_ep + q].astype(jnp.float32)
                for side in range(2):
                    _, kept, away = split(side, 0)
                    part = total[:, side * sub : (side + 1) * sub]
                    if q in away:
                        zout0[side, d, away.index(q)] = part.astype(jnp.bfloat16)
                    else:
                        zown[side, d, kept.index(q)] = part
        z_fold(zout0, zin0, 0)

    def z_fold1():
        arrived(zin0, zfold_recv.at[0])
        for side in range(2):
            _, held, _ = split(side, 0)
            _, kept, away = split(side, 1)
            at_away, at_kept = held.index(away[0]), held.index(kept[0])
            for d in range(2):
                total = zown[side, d, at_away] + zin0[side, d, at_away].astype(jnp.float32)
                zout1[side, d] = total.astype(jnp.bfloat16)
                zown[side, d, at_kept] += zin0[side, d, at_kept].astype(jnp.float32)
        z_fold(zout1, zin1, 1)

    def z_fold2():
        arrived(zin1, zfold_recv.at[1])
        for side in range(2):
            _, held, _ = split(side, 0)
            at_kept = held.index(0)
            cols = slice(side * sub, (side + 1) * sub)
            for d in range(2):
                total = zown[side, d, at_kept] + zin1[side, d].astype(jnp.float32)
                if d:
                    zlast_out[:, cols] = total.astype(jnp.bfloat16)
                else:
                    zlast_keep[:, cols] = total
        send(zlast_out, zlast_in, zlast_send, zlast_recv, sibling)

    def z_finish():
        arrived(zlast_in, zlast_recv)
        put(dp * half + z_block * wide, zlast_keep[...])
        put((1 - dp) * half + z_block * wide, zlast_in[...])

    def finish(n):
        arrived(last_in.at[n], last_recv.at[n])
        for other in range(2):
            value = 0.0 if other else last_keep[n, tp]
            for step in range(n_tp):
                if step or other:
                    value += last_in[n, step * 2 + other - 1].astype(jnp.float32)
            start = (1 - dp if other else dp) * half + n * wide
            put(start, value)

    def stage(n, fn, name):
        if 0 <= n < blocks and n != z_block:
            with jax.named_scope(f"{name}#n={n}"):
                fn(n)

    first = min(2, blocks, pairs)
    for n in range(first):
        with jax.named_scope(f"down_own#n={n}"):
            arrived(dn.at[n], dn_sem.at[n])
            acc[n, :, :wide] = down(n, 0, pairs)
    with jax.named_scope("hidwait"):
        for pair in range(pairs):
            arrived(hid.at[pairs + pair], hid_recv.at[pair])
    for turn in range(blocks + LAGS[2]):
        if turn < blocks:
            with jax.named_scope(f"down#n={turn}"):
                if turn < first:
                    value = down(turn, pairs, 2 * pairs) + acc[turn, :, :wide]
                else:
                    arrived(dn.at[turn], dn_sem.at[turn])
                    value = down(turn, 0, 2 * pairs)
                if turn == z_block:
                    z_store(value)
                else:
                    store0(turn, value)
        stage(turn - LAGS[0], fold1, "fold1")
        stage(turn, fold0, "fold0")
        stage(turn - LAGS[1], fold2, "fold2")
        stage(turn - LAGS[2], finish, "finish")
        for at, fn in zip(Z_TURNS, (z_fold0, z_fold1, z_fold2)):
            if turn == at:
                with jax.named_scope(f"z#n={at}"):
                    fn()
    with jax.named_scope("zfin"):
        z_finish()
    with jax.named_scope("tailsend"):
        arrived(xs.at[:, :, pl.ds(0, groups - 1)], ag_send)
        for kind, ref in enumerate((ids_all, rw_all)):
            arrived(ref.at[pl.ds(rows, total_rows - rows)], small_send.at[kind])
        arrived(hid.at[pl.ds(0, pairs)], hid_send)
        arrived(out0.at[pl.ds(0, blocks - 1)], fold_send.at[0])
        arrived(out1.at[pl.ds(0, blocks - 1)], fold_send.at[1])
        arrived(last_in.at[pl.ds(0, blocks - 1)], last_send)
        arrived(zin, zsend)
        arrived(zout0, zfold_send.at[0])
        arrived(zout1, zfold_send.at[1])
        arrived(zlast_out, zlast_send)
        pltpu.make_async_copy(out_v, out_ref, out_sem).wait()


def fused_plan(mesh, rows, width, local_count, units):
    n_ep, n_dp, n_tp = (mesh.shape[a] for a in ("ep", "dp", "tp"))
    if n_dp != 2 or local_count % 4 or n_ep != 4 or rows % 8 or rows % n_tp:
        return None
    if units % 128 or width % 1024:
        return None
    pairs = local_count // 4
    chunks = width // 1024
    total_rows = 2 * n_ep * rows
    hidden = local_count * units
    slot = 1024 * 4 * units * 2
    pad = -(-(rows // n_tp) // 8) * 8
    held = total_rows * width * 2 + hidden * width + pairs * total_rows * 4 * units * 4
    held += total_rows * hidden * 2 + (total_rows // 2) * (width // 2) * 12
    held += pad * width * (n_tp * 6 + 8 * n_tp) + 5_800_000
    ring = min(chunks * pairs, (VMEM_BYTES - held) // slot)
    if ring < 2 * pairs or pairs < 2 or chunks < 2 or 4 * units < 512:
        return None
    return chunks, pairs, ring


def fused(mesh, plan, tokens, expert_ids, route_weight, gate_weight, up_weight, down_weight):
    chunks, pairs, ring = plan
    n_ep, n_tp = mesh.shape["ep"], mesh.shape["tp"]
    rows, width = tokens.shape
    units = gate_weight.shape[2]
    wide = 512
    blocks = width // 2 // wide
    depth = width // chunks
    total_rows = 2 * n_ep * rows
    out_rows = rows // n_tp
    top = expert_ids.shape[1]
    sub = wide // 2
    dma = pltpu.SemaphoreType.DMA
    f32, bf16 = jnp.float32, jnp.bfloat16
    return pl.pallas_call(
        partial(moe_kernel, n_ep, n_tp, ring, min(EARLY, ring)),
        out_shape=jax.ShapeDtypeStruct((out_rows, width), bf16),
        in_specs=[pl.BlockSpec(memory_space=pltpu.HBM)] * 6,
        out_specs=pl.BlockSpec(memory_space=pltpu.HBM),
        scratch_shapes=[
            pltpu.VMEM((chunks, 2, 2 * n_ep, rows, depth // 2), bf16),
            pltpu.VMEM((top, rows), jnp.int32),
            pltpu.VMEM((top, rows), f32),
            pltpu.VMEM((total_rows, top), jnp.int32),
            pltpu.VMEM((total_rows, top), f32),
            pltpu.VMEM((ring, depth, 4 * units), bf16),
            pltpu.VMEM((blocks, 4 * pairs, units, wide), bf16),
            pltpu.VMEM((pairs, total_rows, 4 * units), f32),
            pltpu.VMEM((2 * pairs, total_rows, 2 * units), bf16),
            pltpu.VMEM((blocks, 2, 2, n_ep // 2, rows, sub), f32),
            pltpu.VMEM((blocks, 2, 2, n_ep // 2, rows, sub), bf16),
            pltpu.VMEM((blocks, 2, 2, n_ep // 2, rows, sub), bf16),
            pltpu.VMEM((blocks, 2, 2, rows, sub), bf16),
            pltpu.VMEM((blocks, 2, 2, rows, sub), bf16),
            pltpu.VMEM((blocks, n_tp, out_rows, wide), f32),
            pltpu.VMEM((blocks, 2, n_tp, out_rows, wide), bf16),
            pltpu.VMEM((blocks, 2 * n_tp - 1, out_rows, wide), bf16),
            pltpu.VMEM((n_tp, 2 * n_ep, out_rows, wide), f32),
            pltpu.VMEM((n_tp, 2 * n_ep, out_rows, wide), bf16),
            pltpu.VMEM((n_tp - 1, 2 * n_ep, out_rows, wide), bf16),
            pltpu.VMEM((2, 2, n_ep // 2, out_rows, sub), f32),
            pltpu.VMEM((2, 2, n_ep // 2, out_rows, sub), bf16),
            pltpu.VMEM((2, 2, n_ep // 2, out_rows, sub), bf16),
            pltpu.VMEM((2, 2, out_rows, sub), bf16),
            pltpu.VMEM((2, 2, out_rows, sub), bf16),
            pltpu.VMEM((out_rows, wide), f32),
            pltpu.VMEM((out_rows, wide), bf16),
            pltpu.VMEM((out_rows, wide), bf16),
            dma((3,)),
            dma((2,)),
            dma((2,)),
            dma,
            dma((chunks, 3)),
            dma((ring,)),
            dma((blocks,)),
            dma,
            dma((pairs,)),
            dma((2,)),
            dma((blocks, 2)),
            dma,
            dma((blocks,)),
            pltpu.VMEM((out_rows, width), bf16),
            dma,
            dma,
            dma,
            dma((2,)),
            dma((2,)),
            dma,
            dma,
        ],
        compiler_params=pltpu.CompilerParams(
            collective_id=0, has_side_effects=True, vmem_limit_bytes=VMEM_BYTES
        ),
    )(tokens, expert_ids.T, route_weight.T, gate_weight, up_weight, down_weight)


def solution(mesh):
    in_specs = (
        P(("ep", "dp"), None),
        P(("ep", "dp"), None),
        P(("ep", "dp"), None),
        P("ep", None, "tp"),
        P("ep", None, "tp"),
        P("ep", "tp", None),
    )
    out_specs = P(("ep", "dp", "tp"), None)

    def body(*arrays):
        rows, width = arrays[0].shape
        local_count, _, units = arrays[3].shape
        plan = fused_plan(mesh, rows, width, local_count, units)
        if plan is None:
            return per_device(*arrays)
        return fused(mesh, plan, *arrays)

    return jax.shard_map(body, mesh=mesh, in_specs=in_specs, out_specs=out_specs, check_vma=False)
```
